32 devices in a mesh: ctx: 16 (over z, y, core), head: 2 (over x).
Axes of the slice: x: 2, y: 2, z: 4, core: 2. Of those that a mesh axis runs over, the one named last changes fastest.
Arguments:
- queries: bfloat16 [16, 1024, 2048], P('ctx', None, 'head'), may hold values from -8 to 8
- keys: bfloat16 [16, 1024, 2048], P('ctx', None, 'head'), may hold values from -8 to 8
- values: bfloat16 [16, 1024, 2048], P('ctx', None, 'head'), may hold values from -24 to 24
- w_out: bfloat16 [2048, 4096], P('head'), may hold values from -0.125 to 0.125
Outputs:
- mixed: bfloat16 [16, 1024, 4096], P('ctx', 'head')
The draws below stay inside these ranges and needn't reach their ends.
All inputs are finite; a program needn't handle non-finite values.
Results may differ from the reference program's by a relative error of at most 0.013.
Values may be sent and summed in bfloat16 or wider, within the bound.
A program may use at most 128 MiB of HBM per device.

```python
import jax
import jax.numpy as jnp
from jax import lax

D = 4096
HD = 128
GROUP = 4
STRIDE = 1024
ROWS = 16
FEAT = 2048
N_HEAD = 2


def draw_queries(key, part):
    shape = (ROWS, STRIDE, FEAT)
    base = jax.random.truncated_normal(jax.random.fold_in(key, 11), -4.0, 4.0, shape, jnp.float32)
    return base.astype(jnp.bfloat16)


def draw_keys(key, part):
    shape = (ROWS, STRIDE, FEAT)
    base = jax.random.truncated_normal(jax.random.fold_in(key, 12), -4.0, 4.0, shape, jnp.float32)
    return base.astype(jnp.bfloat16)


def shard_levels(stream_key, shape, cuts, low, largest):
    level, own = 1.0, jax.random.fold_in(stream_key, 6)
    for dim, blocks in cuts:
        draws = jnp.exp(jax.random.uniform(jax.random.fold_in(own, dim), (blocks,), jnp.float32, low / len(cuts), largest / len(cuts)))
        level = level * jnp.repeat(draws, shape[dim] // blocks).reshape([-1 if axis == dim else 1 for axis in range(len(shape))])
    return level


def noise(stream_key, shape, scale, reach, pieces=(), kind=jnp.bfloat16):
    entries = scale * jax.random.normal(stream_key, shape, jnp.float32)
    if pieces:
        entries = entries * shard_levels(stream_key, shape, pieces, -0.22, 0.18)
    return jnp.clip(entries, -reach, reach).astype(kind)


def setup_inputs(seed: int = 0) -> dict:
    key_of = jax.random.split(jax.random.key(seed), 5)
    queries = draw_queries(jax.random.fold_in(key_of[4], 71), 0)
    keys = draw_keys(jax.random.fold_in(key_of[4], 71), 0)
    values = noise(key_of[2], (ROWS, STRIDE, FEAT), 4.0, 24.0, ((0, 16), (2, 2)))
    w_out = noise(key_of[3], (FEAT, D), FEAT ** -0.5, 0.125, ((0, 2),))
    return {"queries": queries, "keys": keys, "values": values, "w_out": w_out}


masked_score = -1e30


def split_kinds(tensor, parity):
    groups = tensor.shape[2] // (2 * GROUP * HD)
    shaped = tensor.reshape((tensor.shape[0], tensor.shape[1], groups, 2, GROUP, HD))
    return shaped[:, :, :, parity].reshape((tensor.shape[0], tensor.shape[1], groups * GROUP, HD))


def normalized(scores):
    top = jnp.max(scores, axis=-1, keepdims=True)
    expo = jnp.exp(scores - top)
    total = jnp.sum(expo, axis=-1, keepdims=True)
    return (expo / total).astype(jnp.bfloat16)


def reference(queries, keys, values, w_out):
    scale = jnp.float32(1.0 / (HD ** 0.5))
    row_q, row_k, row_v = split_kinds(queries, 0), split_kinds(keys, 0), split_kinds(values, 0)
    col_q, col_k, col_v = split_kinds(queries, 1), split_kinds(keys, 1), split_kinds(values, 1)
    length = STRIDE
    causal_row = lax.broadcasted_iota(jnp.int32, (length, length), 1) <= lax.broadcasted_iota(jnp.int32, (length, length), 0)

    def one_row(triple):
        query_row, key_row, value_row = triple
        scores = jnp.einsum("qhd,khd->hqk", query_row.astype(jnp.float32), key_row.astype(jnp.float32)) * scale
        scores = jnp.where(causal_row, scores, masked_score)
        weights = normalized(scores)
        return jnp.einsum("hqk,khd->qhd", weights.astype(jnp.float32), value_row.astype(jnp.float32)).astype(jnp.bfloat16)

    row_out = lax.map(one_row, (row_q, row_k, row_v))
    causal_col = lax.broadcasted_iota(jnp.int32, (ROWS, ROWS), 1) <= lax.broadcasted_iota(jnp.int32, (ROWS, ROWS), 0)
    scores = jnp.einsum("rchd,schd->chrs", col_q.astype(jnp.float32), col_k.astype(jnp.float32)) * scale
    scores = jnp.where(causal_col, scores, masked_score)
    weights = normalized(scores)
    col_out = jnp.einsum("chrs,schd->rchd", weights.astype(jnp.float32), col_v.astype(jnp.float32)).astype(jnp.bfloat16)
    groups = FEAT // (2 * GROUP * HD)
    joined = jnp.stack([row_out.reshape((ROWS, STRIDE, groups, GROUP, HD)), col_out.reshape((ROWS, STRIDE, groups, GROUP, HD))], axis=3)
    flat = joined.reshape((ROWS * STRIDE, FEAT))
    width = FEAT // N_HEAD
    total = jnp.zeros((ROWS * STRIDE, D), jnp.float32)
    for index in range(N_HEAD):
        term = jnp.dot(flat[:, index * width:(index + 1) * width], w_out[index * width:(index + 1) * width], preferred_element_type=jnp.float32)
        total = total + lax.optimization_barrier(term.astype(jnp.bfloat16)).astype(jnp.float32)
    return total.astype(jnp.bfloat16).reshape((ROWS, STRIDE, D))
```

```python
import functools

import jax
import jax.numpy as jnp
from jax import lax
from jax.experimental import pallas as pl
from jax.experimental.pallas import tpu as pltpu
from jax.sharding import PartitionSpec as P

HD = 128
GROUP = 4
MESH = pl.DeviceIdType.MESH
PIECES = 4

masked_score = -1e30


def attend(query, key, value, allowed):
    scores = lax.dot_general(
        query, key, (((1,), (1,)), ((), ())), preferred_element_type=jnp.float32
    ) * jnp.float32(1.0 / HD**0.5)
    scores = jnp.where(allowed, scores, masked_score)
    top = jnp.max(scores, axis=-1, keepdims=True)
    expo = jnp.exp(scores - top)
    total = jnp.sum(expo, axis=-1, keepdims=True)
    mixed = jnp.dot(expo.astype(jnp.bfloat16), value, preferred_element_type=jnp.float32)
    return (mixed / total).astype(jnp.bfloat16)


def body(
    n, q_hbm, k_hbm, v_hbm, w_hbm, out_ref, q_row, k_row, v_row, q_col, k_col, v_col,
    col_out, row_out, joined, w_own, w_other, local_sem, in_send, in_recv, back_send, back_recv,
    w_send, w_recv, row_send, row_recv,
):
    me, head = lax.axis_index("ctx"), lax.axis_index("head")
    other = 1 - head
    stride = q_hbm.shape[1]
    block = q_row.shape[1]
    depth = w_own.shape[0]
    half = joined.shape[1]
    cols = stride // n
    hbm = (q_hbm, k_hbm, v_hbm)
    rows_in = (q_row, k_row, v_row)
    cols_in = (q_col, k_col, v_col)
    back_head = lax.div(me * cols, half)
    member = lax.rem(me, 4)
    sibling = me + 1 - 2 * lax.rem(me, 2)
    beside = me + 2 - 4 * lax.div(member, 2)
    piece = depth // (4 * PIECES)

    def col_copy(t, d):
        peer = lax.rem(me + d, n)
        return pltpu.make_async_remote_copy(
            src_ref=hbm[t].at[0, pl.ds(peer * cols, cols), pl.ds(block, block)],
            dst_ref=cols_in[t].at[me],
            send_sem=in_send.at[t, d],
            recv_sem=in_recv.at[t, d],
            device_id=(peer, head),
            device_id_type=MESH,
        )

    def col_arrival(t, d):
        source = lax.rem(me + n - d, n)
        return pltpu.make_async_remote_copy(
            src_ref=hbm[t].at[0, pl.ds(0, cols), pl.ds(block, block)],
            dst_ref=cols_in[t].at[source],
            send_sem=in_send.at[t, d],
            recv_sem=in_recv.at[t, d],
            device_id=(source, head),
            device_id_type=MESH,
        )

    def w_copy(source, index, way, to_ctx, to_head):
        rows = pl.ds(index * piece, piece)
        return pltpu.make_async_remote_copy(
            src_ref=source.at[rows],
            dst_ref=w_other.at[rows],
            send_sem=w_send.at[way, index],
            recv_sem=w_recv.at[index],
            device_id=(to_ctx, to_head),
            device_id_type=MESH,
        )

    def index_of(who, s):
        return who * PIECES + s

    member_sibling = lax.rem(sibling, 4)
    member_beside = lax.rem(beside, 4)
    member_far = lax.rem(member + 2, 4) + 1 - 2 * lax.rem(member, 2)

    for t in range(3):

        @pl.loop(1, n)
        def _(d):
            col_copy(t, d).start()

    @pl.loop(0, PIECES)
    def _(s):
        w_copy(w_hbm, index_of(member, s), 0, me, other).start()

    local = [
        pltpu.make_async_copy(hbm[t].at[0, :, pl.ds(0, block)], rows_in[t], local_sem.at[t])
        for t in range(3)
    ]
    local += [
        pltpu.make_async_copy(
            hbm[t].at[0, pl.ds(me * cols, cols), pl.ds(block, block)],
            cols_in[t].at[me],
            local_sem.at[3 + t],
        )
        for t in range(3)
    ]
    local.append(pltpu.make_async_copy(w_hbm, w_own, local_sem.at[6]))
    for copy in local:
        copy.start()
    for copy in local[:3]:
        copy.wait()

    tile = min(256, half)
    row_index = lax.broadcasted_iota(jnp.int32, (tile, stride), 0)
    key_index = lax.broadcasted_iota(jnp.int32, (tile, stride), 1)

    @pl.loop(0, block // HD)
    def _(h):
        lanes = pl.ds(pl.multiple_of(h * HD, HD), HD)
        for start in range(0, stride, tile):
            end = start + tile
            row_out[pl.ds(start, tile), lanes] = attend(
                q_row[pl.ds(start, tile), lanes],
                k_row[pl.ds(0, end), lanes],
                v_row[pl.ds(0, end), lanes],
                key_index[:, :end] <= row_index[:, :end] + start,
            )

    row_copy = pltpu.make_async_remote_copy(
        src_ref=row_out.at[pl.ds(pl.multiple_of(other * half, half), half)],
        dst_ref=joined.at[head, :, pl.ds(0, block)],
        send_sem=row_send,
        recv_sem=row_recv,
        device_id=(me, other),
        device_id_type=MESH,
    )
    row_copy.start()
    joined[head, :, pl.ds(0, block)] = row_out[pl.ds(pl.multiple_of(head * half, half), half)]

    @pl.loop(0, PIECES)
    def _(s):
        index = index_of(member, s)
        w_copy(w_hbm, index, 0, me, other).wait_recv()
        w_copy(w_other, index, 1, beside, head).start()
        w_copy(w_other, index, 2, sibling, head).start()

    for copy in local[3:]:
        copy.wait()
    for t in range(3):

        @pl.loop(1, n)
        def _(d):
            col_arrival(t, d).wait_recv()

    width = min(cols, max(16, 256 // n))
    size = n * width
    r_index = lax.broadcasted_iota(jnp.int32, (size, size), 0)
    s_index = lax.broadcasted_iota(jnp.int32, (size, size), 1)
    allowed = (s_index <= r_index) & (((r_index - s_index) & (width - 1)) == 0)

    @pl.loop(0, block // HD)
    def _(h):
        lanes = pl.ds(pl.multiple_of(h * HD, HD), HD)
        for start in range(0, cols, width):
            at = (slice(None), pl.ds(start, width), lanes)
            got = attend(*(ref[at].reshape(size, HD) for ref in cols_in), allowed)
            col_out[at] = got.reshape(n, width, HD)

    def back_copy(r):
        slot = lax.rem(me, n // 2)
        return pltpu.make_async_remote_copy(
            src_ref=col_out.at[r],
            dst_ref=joined.at[head, pl.ds(pl.multiple_of(slot * cols, cols), cols), pl.ds(block, block)],
            send_sem=back_send.at[r],
            recv_sem=back_recv.at[head, slot],
            device_id=(r, back_head),
            device_id_type=MESH,
        )

    def back_arrival(source_head, slot):
        return pltpu.make_async_remote_copy(
            src_ref=col_out.at[0],
            dst_ref=joined.at[
                source_head, pl.ds(pl.multiple_of(slot * cols, cols), cols), pl.ds(block, block)
            ],
            send_sem=back_send.at[0],
            recv_sem=back_recv.at[source_head, slot],
            device_id=(me, other),
            device_id_type=MESH,
        )

    stays = back_head == head

    @pl.loop(1, n)
    def _(d):
        back_copy(lax.rem(me + d, n)).start()

    @pl.when(stays)
    def _():
        slot = lax.rem(me, n // 2)
        joined[head, pl.ds(pl.multiple_of(slot * cols, cols), cols), pl.ds(block, block)] = col_out[me]

    @pl.when(jnp.logical_not(stays))
    def _():
        back_copy(me).start()

    @pl.loop(0, PIECES)
    def _(s):
        index = index_of(member_beside, s)
        w_copy(w_other, index, 1, beside, head).wait_recv()
        w_copy(w_other, index, 3, sibling, head).start()

    row_copy.wait_recv()

    @pl.loop(0, PIECES)
    def _(s):
        w_copy(w_other, index_of(member_sibling, s), 2, sibling, head).wait_recv()
        w_copy(w_other, index_of(member_far, s), 3, sibling, head).wait_recv()

    for source_head in range(2):

        @pl.loop(0, n // 2)
        def _(slot):
            mine = (head * (n // 2) + slot == me) & (head == source_head)

            @pl.when(jnp.logical_not(mine))
            def _():
                back_arrival(source_head, slot).wait_recv()

    step = 512

    @pl.loop(0, out_ref.shape[1] // step)
    def _(c):
        lanes = pl.ds(pl.multiple_of(c * step, step), step)
        total = jnp.dot(joined[head], w_own[:, lanes], preferred_element_type=jnp.float32)
        total += jnp.dot(joined[other], w_other[:, lanes], preferred_element_type=jnp.float32)
        out_ref[:, lanes] = total.astype(jnp.bfloat16)

    for t in range(3):

        @pl.loop(1, n)
        def _(d):
            col_copy(t, d).wait_send()

    @pl.loop(0, PIECES)
    def _(s):
        w_copy(w_hbm, index_of(member, s), 0, me, other).wait_send()
        w_copy(w_other, index_of(member, s), 1, beside, head).wait_send()
        w_copy(w_other, index_of(member, s), 2, sibling, head).wait_send()
        w_copy(w_other, index_of(member_beside, s), 3, sibling, head).wait_send()

    row_copy.wait_send()

    @pl.loop(1, n)
    def _(d):
        back_copy(lax.rem(me + d, n)).wait_send()

    @pl.when(jnp.logical_not(stays))
    def _():
        back_copy(me).wait_send()


def on_device(n, queries, keys, values, w_out):
    _, stride, local_feat = queries.shape
    depth, model_width = w_out.shape
    block = GROUP * HD
    assert queries.shape[0] == 1 and local_feat == 2 * block
    half = stride // lax.axis_size("head")
    cols = stride // n
    bf16 = jnp.bfloat16
    dma = pltpu.SemaphoreType.DMA
    out = pl.pallas_call(
        functools.partial(body, n),
        out_shape=jax.ShapeDtypeStruct((half, model_width), bf16),
        in_specs=[pl.BlockSpec(memory_space=pltpu.HBM)] * 4,
        out_specs=pl.BlockSpec(memory_space=pltpu.VMEM),
        scratch_shapes=[pltpu.VMEM((stride, block), bf16)] * 3
        + [pltpu.VMEM((n, cols, block), bf16)] * 4
        + [
            pltpu.VMEM((stride, block), bf16),
            pltpu.VMEM((2, half, local_feat), bf16),
            pltpu.VMEM((depth, model_width), bf16),
            pltpu.VMEM((depth, model_width), bf16),
            dma((7,)),
            dma((3, n)),
            dma((3, n)),
            dma((n,)),
            dma((2, n // 2)),
            dma((4, 4 * PIECES)),
            dma((4 * PIECES,)),
            dma,
            dma,
        ],
        compiler_params=pltpu.CompilerParams(has_side_effects=True, vmem_limit_bytes=60 * 2**20),
    )(queries, keys, values, w_out)
    return out.reshape((1, half, model_width))


def solution(mesh):
    return jax.shard_map(
        functools.partial(on_device, mesh.shape["ctx"]),
        mesh=mesh,
        in_specs=(
            P("ctx", None, "head"),
            P("ctx", None, "head"),
            P("ctx", None, "head"),
            P("head", None),
        ),
        out_specs=P("ctx", "head", None),
        check_vma=False,
    )
```

```python
import functools

import jax
import jax.numpy as jnp
from jax import lax
from jax.experimental import pallas as pl
from jax.experimental.pallas import tpu as pltpu
from jax.sharding import PartitionSpec as P

HD = 128
GROUP = 4
MESH = pl.DeviceIdType.MESH
PIECES = 8
STRAIGHT = 2
PARTS = 2

masked_score = -1e30


def attend(query, key, value, allowed):
    scores = lax.dot_general(
        query, key, (((1,), (1,)), ((), ())), preferred_element_type=jnp.float32
    ) * jnp.float32(1.0 / HD**0.5)
    scores = jnp.where(allowed, scores, masked_score)
    top = jnp.max(scores, axis=-1, keepdims=True)
    expo = jnp.exp(scores - top)
    total = jnp.sum(expo, axis=-1, keepdims=True)
    mixed = jnp.dot(expo.astype(jnp.bfloat16), value, preferred_element_type=jnp.float32)
    return (mixed / total).astype(jnp.bfloat16)


def body(
    n, q_hbm, k_hbm, v_hbm, w_hbm, out_ref, q_row, k_row, v_row, q_col, k_col, v_col,
    col_out, row_out, joined, summed, w_own, w_other, local_sem, in_send, in_recv, back_send, back_recv,
    w_send, w_recv, row_send, row_recv,
):
    me, head = lax.axis_index("ctx"), lax.axis_index("head")
    other = 1 - head
    stride = q_hbm.shape[1]
    block = q_row.shape[1]
    depth = w_own.shape[0]
    half = joined.shape[1]
    cols = stride // n
    share = block // PARTS
    hbm = (q_hbm, k_hbm, v_hbm)
    rows_in = (q_row, k_row, v_row)
    cols_in = (q_col, k_col, v_col)
    back_head = lax.div(me * cols, half)
    member = lax.rem(me, 4)
    sibling = me + 1 - 2 * lax.rem(me, 2)
    beside = me + 2 - 4 * lax.div(member, 2)
    piece = depth // (4 * PIECES)

    def col_copy(t, part, d):
        peer = lax.rem(me + d, n)
        lanes = pl.ds(part * share, share)
        return pltpu.make_async_remote_copy(
            src_ref=hbm[t].at[0, pl.ds(peer * cols, cols), pl.ds(block + part * share, share)],
            dst_ref=cols_in[t].at[me, :, lanes],
            send_sem=in_send.at[t * PARTS + part, d],
            recv_sem=in_recv.at[t * PARTS + part, d],
            device_id=(peer, head),
            device_id_type=MESH,
        )

    def col_arrival(t, part, d):
        source = lax.rem(me + n - d, n)
        lanes = pl.ds(part * share, share)
        return pltpu.make_async_remote_copy(
            src_ref=hbm[t].at[0, pl.ds(0, cols), pl.ds(block + part * share, share)],
            dst_ref=cols_in[t].at[source, :, lanes],
            send_sem=in_send.at[t * PARTS + part, d],
            recv_sem=in_recv.at[t * PARTS + part, d],
            device_id=(source, head),
            device_id_type=MESH,
        )

    def w_copy(source, index, way, to_ctx, to_head):
        rows = pl.ds(index * piece, piece)
        return pltpu.make_async_remote_copy(
            src_ref=source.at[rows],
            dst_ref=w_other.at[rows],
            send_sem=w_send.at[way, index],
            recv_sem=w_recv.at[index],
            device_id=(to_ctx, to_head),
            device_id_type=MESH,
        )

    def index_of(who, s):
        return who * PIECES + s

    member_sibling = lax.rem(sibling, 4)
    member_beside = lax.rem(beside, 4)
    member_far = lax.rem(member + 2, 4) + 1 - 2 * lax.rem(member, 2)

    for part in range(PARTS):

        @pl.loop(1, n)
        def _(d):
            for t in range(3):
                col_copy(t, part, d).start()

    @pl.loop(0, PIECES)
    def _(s):
        w_copy(w_hbm, index_of(member, s), 0, me, other).start()

    @pl.loop(PIECES - STRAIGHT, PIECES)
    def _(s):
        w_copy(w_hbm, index_of(member_beside, s), 0, me, other).start()

    local = [
        pltpu.make_async_copy(hbm[t].at[0, :, pl.ds(0, block)], rows_in[t], local_sem.at[t])
        for t in range(3)
    ]
    local += [
        pltpu.make_async_copy(
            hbm[t].at[0, pl.ds(me * cols, cols), pl.ds(block, block)],
            cols_in[t].at[me],
            local_sem.at[3 + t],
        )
        for t in range(3)
    ]
    local.append(pltpu.make_async_copy(w_hbm, w_own, local_sem.at[6]))
    for copy in local:
        copy.start()
    for copy in local[:3]:
        copy.wait()

    tile = min(256, half)
    row_index = lax.broadcasted_iota(jnp.int32, (tile, stride), 0)
    key_index = lax.broadcasted_iota(jnp.int32, (tile, stride), 1)

    @pl.loop(0, block // HD)
    def _(h):
        lanes = pl.ds(pl.multiple_of(h * HD, HD), HD)
        for start in range(0, stride, tile):
            end = start + tile
            row_out[pl.ds(start, tile), lanes] = attend(
                q_row[pl.ds(start, tile), lanes],
                k_row[pl.ds(0, end), lanes],
                v_row[pl.ds(0, end), lanes],
                key_index[:, :end] <= row_index[:, :end] + start,
            )

    row_copy = pltpu.make_async_remote_copy(
        src_ref=row_out.at[pl.ds(pl.multiple_of(other * half, half), half)],
        dst_ref=joined.at[head, :, pl.ds(0, block)],
        send_sem=row_send,
        recv_sem=row_recv,
        device_id=(me, other),
        device_id_type=MESH,
    )
    row_copy.start()
    joined[head, :, pl.ds(0, block)] = row_out[pl.ds(pl.multiple_of(head * half, half), half)]

    def onward(first, last):
        @pl.loop(first, last)
        def _(s):
            index = index_of(member, s)
            w_copy(w_hbm, index, 0, me, other).wait_recv()

            @pl.when(s < PIECES - STRAIGHT)
            def _():
                w_copy(w_other, index, 1, beside, head).start()

            w_copy(w_other, index, 2, sibling, head).start()

    onward(0, PIECES // 2)

    for copy in local[3:]:
        copy.wait()

    step = 512

    def tiles(add):
        @pl.loop(0, out_ref.shape[1] // step)
        def _(c):
            add(pl.ds(pl.multiple_of(c * step, step), step))

    def own_row_part(lanes):
        summed[:, lanes] = jnp.dot(
            joined[head, :, pl.ds(0, block)],
            w_own[pl.ds(0, block), lanes],
            preferred_element_type=jnp.float32,
        )

    tiles(own_row_part)
    width = min(cols, max(16, 256 // n))
    size = n * width
    r_index = lax.broadcasted_iota(jnp.int32, (size, size), 0)
    s_index = lax.broadcasted_iota(jnp.int32, (size, size), 1)
    allowed = (s_index <= r_index) & (((r_index - s_index) & (width - 1)) == 0)

    slot_here = lax.rem(me, n // 2)
    stays = back_head == head

    def landing(source_head, part, slot):
        return joined.at[
            source_head,
            pl.ds(pl.multiple_of(slot * cols, cols), cols),
            pl.ds(block + part * share, share),
        ]

    def back_copy(part, r):
        return pltpu.make_async_remote_copy(
            src_ref=col_out.at[r, :, pl.ds(part * share, share)],
            dst_ref=landing(head, part, slot_here),
            send_sem=back_send.at[part, r],
            recv_sem=back_recv.at[head * PARTS + part, slot_here],
            device_id=(r, back_head),
            device_id_type=MESH,
        )

    def back_arrival(source_head, part, slot):
        return pltpu.make_async_remote_copy(
            src_ref=col_out.at[0, :, pl.ds(part * share, share)],
            dst_ref=landing(source_head, part, slot),
            send_sem=back_send.at[part, 0],
            recv_sem=back_recv.at[source_head * PARTS + part, slot],
            device_id=(me, other),
            device_id_type=MESH,
        )

    for part in range(PARTS):

        @pl.loop(1, n)
        def _(d):
            for t in range(3):
                col_arrival(t, part, d).wait_recv()

        @pl.loop(part * (share // HD), (part + 1) * (share // HD))
        def _(h):
            lanes = pl.ds(pl.multiple_of(h * HD, HD), HD)
            for start in range(0, cols, width):
                at = (slice(None), pl.ds(start, width), lanes)
                got = attend(*(ref[at].reshape(size, HD) for ref in cols_in), allowed)
                col_out[at] = got.reshape(n, width, HD)

        @pl.loop(1, n)
        def _(d):
            back_copy(part, lax.rem(me + d, n)).start()

        @pl.when(stays)
        def _():
            rows = pl.ds(pl.multiple_of(slot_here * cols, cols), cols)
            joined[head, rows, pl.ds(block + part * share, share)] = col_out[
                me, :, pl.ds(part * share, share)
            ]

        @pl.when(jnp.logical_not(stays))
        def _():
            back_copy(part, me).start()

        if part == 0:
            onward(PIECES // 2, PIECES)

    @pl.loop(0, PIECES)
    def _(s):
        index = index_of(member_beside, s)
        w_copy(w_other, index, 1, beside, head).wait_recv()
        w_copy(w_other, index, 3, sibling, head).start()

    row_copy.wait_recv()

    def back_wait(source_head):
        @pl.loop(0, n // 2)
        def _(slot):
            mine = (head * (n // 2) + slot == me) & (head == source_head)

            @pl.when(jnp.logical_not(mine))
            def _():
                for part in range(PARTS):
                    back_arrival(source_head, part, slot).wait_recv()

    back_wait(head)

    def own_col_part(lanes):
        summed[:, lanes] += jnp.dot(
            joined[head, :, pl.ds(block, block)],
            w_own[pl.ds(block, block), lanes],
            preferred_element_type=jnp.float32,
        )

    tiles(own_col_part)

    @pl.loop(0, PIECES)
    def _(s):
        w_copy(w_other, index_of(member_sibling, s), 2, sibling, head).wait_recv()
        w_copy(w_other, index_of(member_far, s), 3, sibling, head).wait_recv()

    back_wait(other)

    def other_part(lanes):
        total = summed[:, lanes] + jnp.dot(
            joined[other], w_other[:, lanes], preferred_element_type=jnp.float32
        )
        out_ref[:, lanes] = total.astype(jnp.bfloat16)

    tiles(other_part)

    for part in range(PARTS):

        @pl.loop(1, n)
        def _(d):
            for t in range(3):
                col_copy(t, part, d).wait_send()

    @pl.loop(0, PIECES)
    def _(s):
        w_copy(w_hbm, index_of(member, s), 0, me, other).wait_send()
        w_copy(w_other, index_of(member, s), 2, sibling, head).wait_send()
        w_copy(w_other, index_of(member_beside, s), 3, sibling, head).wait_send()

    @pl.loop(0, PIECES - STRAIGHT)
    def _(s):
        w_copy(w_other, index_of(member, s), 1, beside, head).wait_send()

    @pl.loop(PIECES - STRAIGHT, PIECES)
    def _(s):
        w_copy(w_hbm, index_of(member_beside, s), 0, me, other).wait_send()

    row_copy.wait_send()

    for part in range(PARTS):

        @pl.loop(1, n)
        def _(d):
            back_copy(part, lax.rem(me + d, n)).wait_send()

        @pl.when(jnp.logical_not(stays))
        def _():
            back_copy(part, me).wait_send()


def on_device(n, queries, keys, values, w_out):
    _, stride, local_feat = queries.shape
    depth, model_width = w_out.shape
    block = GROUP * HD
    assert queries.shape[0] == 1 and local_feat == 2 * block
    half = stride // lax.axis_size("head")
    cols = stride // n
    bf16 = jnp.bfloat16
    dma = pltpu.SemaphoreType.DMA
    out = pl.pallas_call(
        functools.partial(body, n),
        out_shape=jax.ShapeDtypeStruct((half, model_width), bf16),
        in_specs=[pl.BlockSpec(memory_space=pltpu.HBM)] * 4,
        out_specs=pl.BlockSpec(memory_space=pltpu.VMEM),
        scratch_shapes=[pltpu.VMEM((stride, block), bf16)] * 3
        + [pltpu.VMEM((n, cols, block), bf16)] * 4
        + [
            pltpu.VMEM((stride, block), bf16),
            pltpu.VMEM((2, half, local_feat), bf16),
            pltpu.VMEM((half, model_width), jnp.float32),
            pltpu.VMEM((depth, model_width), bf16),
            pltpu.VMEM((depth, model_width), bf16),
            dma((7,)),
            dma((3 * PARTS, n)),
            dma((3 * PARTS, n)),
            dma((PARTS, n)),
            dma((2 * PARTS, n // 2)),
            dma((4, 4 * PIECES)),
            dma((4 * PIECES,)),
            dma,
            dma,
        ],
        compiler_params=pltpu.CompilerParams(has_side_effects=True, vmem_limit_bytes=60 * 2**20),
    )(queries, keys, values, w_out)
    return out.reshape((1, half, model_width))


def solution(mesh):
    return jax.shard_map(
        functools.partial(on_device, mesh.shape["ctx"]),
        mesh=mesh,
        in_specs=(
            P("ctx", None, "head"),
            P("ctx", None, "head"),
            P("ctx", None, "head"),
            P("head", None),
        ),
        out_specs=P("ctx", "head", None),
        check_vma=False,
    )
```
